256 devices in a mesh: scan: 4 (over x, y), row: 64 (over z, core).
Axes of the slice: x: 2, y: 2, z: 32, core: 2. Of those that a mesh axis runs over, the one named last changes fastest.
The devices are a block of a 4x8x32 slice.
Arguments:
- object_field: float32 [2, 2, 32768, 768], P(None, None, ('scan', 'row')), parts along dimension 2, may hold values from -1 to 1
- row_offset: int32 [256], P(('scan', 'row')), parts along dimension 0, may hold values from 0 to 127
- col_offset: int32 [256], P(('scan', 'row')), parts along dimension 0, may hold values from 0 to 256
- amplitudes: float32 [256, 512, 512], P(('scan', 'row')), parts along dimension 0, may hold values from 0.2 to 2
- probe: float32 [8, 512, 512], P('scan'), parts along dimension 0, may hold values from -6 to 6
- phase: float32 [512, 512], replicated, may hold values from -3.140625 to 3.140625
Outputs:
- updated_object: float32 [2, 2, 32768, 768], P(None, None, ('scan', 'row')), parts along dimension 2
The draws below stay inside these ranges and needn't reach their ends.
There are 4 independent parts, one for each index of `scan`. The reference program is written for one: setup_inputs(seed, part) draws one part's arguments, and reference() takes and returns one part's arrays. A program takes and returns all parts, laid end to end along the dimension named above; an argument that names none is the same for every part. Nothing has to cross between parts.
All inputs are finite; a program needn't handle non-finite values.
Results may differ from the reference program's by a relative error of at most 0.014.
Values sent between devices are 32-bit elements; how exact they have to be, the bound alone decides.
No kernel may reach another device: no remote copies, remote signals or barrier semaphores. Data moves between devices by JAX's collectives and lax.ppermute only.
A program may use at most 64 MiB of HBM per device.

```python
import math
import jax
import jax.numpy as jnp
from jax import lax

P_SIZE = 512
STRIP = 128
COLS = 768
NY = 8192
N_ROW = 64


def plant(array, stream_key, low, high):
    longest = array.shape.index(max(array.shape))
    spots = []
    for shift in (0, 1):
        where = [jax.random.randint(jax.random.fold_in(stream_key, axis), (), 0, length) for axis, length in enumerate(array.shape)]
        where[longest] = (where[longest] + shift) % array.shape[longest]
        spots.append(tuple(where))
    return array.at[spots[0]].set(low).at[spots[1]].set(high)


def steps_of(rng, shape, pieces, smallest, top_value):
    gain, own = 1.0, jax.random.fold_in(rng, 6)
    for axis_at, shards_of in pieces:
        heights = jnp.exp(jax.random.uniform(jax.random.fold_in(own, axis_at), (shards_of,), jnp.float32, smallest / len(pieces), top_value / len(pieces)))
        gain = gain * jnp.repeat(heights, shape[axis_at] // shards_of).reshape([-1 if axis == axis_at else 1 for axis in range(len(shape))])
    return gain


def scatter_about(rng, shape, scale, limit, kind=jnp.bfloat16):
    result = scale * jax.random.normal(rng, shape, jnp.float32)
    return jnp.clip(result, min=-limit, max=limit).astype(kind)


def setup_inputs(seed: int = 0, part: int = 0) -> dict:
    arg_keys = jax.random.split(jax.random.key(seed), 7)
    part_splits = jax.random.split(jax.random.fold_in(arg_keys[6], part), 7)
    object_field = jnp.clip(jax.random.uniform(part_splits[0], (2, 2, NY, COLS), jnp.float32, -1.0, 1.0) * steps_of(part_splits[0], (2, 2, NY, COLS), ((2, 64),), -0.4, 0.0), -1.0, 1.0)
    row_offset = plant(jax.random.randint(part_splits[1], (N_ROW,), 0, STRIP), jax.random.fold_in(part_splits[1], 1), 0, STRIP - 1).astype(jnp.int32)
    col_offset = plant(jax.random.randint(part_splits[2], (N_ROW,), 0, COLS - P_SIZE + 1), jax.random.fold_in(part_splits[2], 1), 0, COLS - P_SIZE).astype(jnp.int32)
    amplitudes = jnp.clip(0.2 + 1.8 * jax.random.uniform(part_splits[3], (N_ROW, P_SIZE, P_SIZE), jnp.float32) ** steps_of(part_splits[3], (N_ROW, P_SIZE, P_SIZE), ((0, 64),), -0.2, 0.2), 0.2, 2.0)
    probe = scatter_about(part_splits[4], (2, P_SIZE, P_SIZE), 1.0, 6.0, jnp.float32)
    phase = jnp.clip(jax.random.uniform(arg_keys[5], (P_SIZE, P_SIZE), jnp.float32, -3.140625, 3.140625), -3.140625, 3.140625)
    return {"object_field": object_field, "row_offset": row_offset, "col_offset": col_offset, "amplitudes": amplitudes, "probe": probe, "phase": phase}


def dft_mats(length, flip):
    index = jnp.arange(length, dtype=jnp.int32)
    angles = (index[:, None] * index[None, :] % length).astype(jnp.float32) * (-2.0 * math.pi / length)
    factor = 1.0 / math.sqrt(length)
    cos_table = (jnp.cos(angles) * factor).astype(jnp.bfloat16)
    sin_table = (jnp.sin(angles) * factor).astype(jnp.bfloat16)
    if flip:
        sin_table = -sin_table
    left_real = jnp.concatenate([cos_table, -sin_table], axis=1)
    left_imag = jnp.concatenate([sin_table, cos_table], axis=1)
    right_real = jnp.concatenate([cos_table, -sin_table], axis=0)
    right_imag = jnp.concatenate([sin_table, cos_table], axis=0)
    return (left_real, left_imag, right_real, right_imag)

def transform(real_part, imag_part, mats):
    left_real, left_imag, right_real, right_imag = mats
    stacked = jnp.concatenate([real_part.astype(jnp.bfloat16), imag_part.astype(jnp.bfloat16)], axis=0)
    half_real = jnp.dot(left_real, stacked, preferred_element_type=jnp.float32).astype(jnp.bfloat16)
    half_imag = jnp.dot(left_imag, stacked, preferred_element_type=jnp.float32).astype(jnp.bfloat16)
    joined = jnp.concatenate([half_real, half_imag], axis=1)
    return (jnp.dot(joined, right_real, preferred_element_type=jnp.float32), jnp.dot(joined, right_imag, preferred_element_type=jnp.float32))

def cmul(a_real, a_imag, b_real, b_imag):
    return (a_real * b_real - a_imag * b_imag, a_real * b_imag + a_imag * b_real)

def cmul_conj(a_real, a_imag, b_real, b_imag):
    return (a_real * b_real + a_imag * b_imag, a_real * b_imag - a_imag * b_real)

def window_gradient(window, probe, amplitude, phase, forward, inverse):
    prop_real = jnp.cos(phase)
    prop_imag = jnp.sin(phase)
    probe_real, probe_imag = (probe[0], probe[1])
    first_real, first_imag = (window[0, 0], window[0, 1])
    second_real, second_imag = (window[1, 0], window[1, 1])
    exit_real, exit_imag = cmul(probe_real, probe_imag, first_real, first_imag)
    freq_real, freq_imag = transform(exit_real, exit_imag, forward)
    moved_real, moved_imag = cmul(freq_real, freq_imag, prop_real, prop_imag)
    inner_real, inner_imag = transform(moved_real, moved_imag, inverse)
    wave_real, wave_imag = cmul(inner_real, inner_imag, second_real, second_imag)
    far_real, far_imag = transform(wave_real, wave_imag, forward)
    modulus = jnp.sqrt(far_real * far_real + far_imag * far_imag)
    ratio = amplitude / jnp.maximum(modulus, 0.1)
    resid_real = far_real * (1.0 - ratio)
    resid_imag = far_imag * (1.0 - ratio)
    back_real, back_imag = transform(resid_real, resid_imag, inverse)
    grad2_real, grad2_imag = cmul_conj(inner_real, inner_imag, back_real, back_imag)
    mid_real, mid_imag = cmul_conj(second_real, second_imag, back_real, back_imag)
    spec_real, spec_imag = transform(mid_real, mid_imag, forward)
    unprop_real, unprop_imag = cmul_conj(prop_real, prop_imag, spec_real, spec_imag)
    entry_real, entry_imag = transform(unprop_real, unprop_imag, inverse)
    grad1_real, grad1_imag = cmul_conj(probe_real, probe_imag, entry_real, entry_imag)
    return jnp.stack([jnp.stack([grad1_real, grad1_imag]), jnp.stack([grad2_real, grad2_imag])])

def reference(object_field, row_offset, col_offset, amplitudes, probe, phase):
    forward = dft_mats(P_SIZE, False)
    inverse = dft_mats(P_SIZE, True)
    span = jnp.arange(P_SIZE, dtype=jnp.int32)

    def window_rows(device, offset):
        return (device * STRIP + offset + STRIP // 2 - 2 * STRIP + span + NY) % NY

    def one_device(items):
        device, offset, column, amplitude = items
        rows = window_rows(device, offset)
        taken = jnp.take(object_field, rows, axis=2)
        window = lax.dynamic_slice_in_dim(taken, column, P_SIZE, axis=3)
        return window_gradient(window, probe, amplitude, phase, forward, inverse)
    devices = jnp.arange(N_ROW, dtype=jnp.int32)
    grads = lax.map(one_device, (devices, row_offset, col_offset, amplitudes))

    def place(device, canvas):
        rows = window_rows(device, row_offset[device])
        columns = col_offset[device] + span
        return canvas.at[:, :, rows[:, None], columns[None, :]].add(grads[device])
    canvas = lax.fori_loop(0, N_ROW, place, jnp.zeros_like(object_field))
    return object_field - 0.5 * canvas
```

```python
import math

import jax
import jax.numpy as jnp
from jax import lax
from jax.sharding import PartitionSpec as P


def hop(block, route):
    size = lax.axis_size("row")
    pairs = [(i, route(i) % size) for i in range(size) if route(i) is not None]
    return lax.ppermute(block, "row", pairs)


def shift(block, distance):
    return hop(block, lambda i: i + distance)


def swap(block):
    return hop(block, lambda i: i ^ 1)


def base_tables(length):
    index = jnp.arange(length, dtype=jnp.int32)
    angles = (index[:, None] * index[None, :] % length).astype(jnp.float32) * (
        -2.0 * math.pi / length
    )
    factor = 1.0 / math.sqrt(length)
    return (
        (jnp.cos(angles) * factor).astype(jnp.bfloat16),
        (jnp.sin(angles) * factor).astype(jnp.bfloat16),
    )


def rolled(table, amount, axis):
    length = table.shape[axis]
    doubled = jnp.concatenate([table, table], axis=axis)
    start = lax.rem(length - amount, length)
    return lax.dynamic_slice_in_dim(doubled, start, length, axis)


def product(left, right):
    return jnp.dot(left, right, preferred_element_type=jnp.float32)


def transform(real_part, imag_part, mats):
    left_real, left_imag, right_real, right_imag = mats
    stacked = jnp.concatenate(
        [real_part.astype(jnp.bfloat16), imag_part.astype(jnp.bfloat16)], axis=0
    )
    half_real = product(left_real, stacked).astype(jnp.bfloat16)
    half_imag = product(left_imag, stacked).astype(jnp.bfloat16)
    joined = jnp.concatenate([half_real, half_imag], axis=1)
    return product(joined, right_real), product(joined, right_imag)


def transform_tables(cos_left, sin_left, cos_right, sin_right):
    return (
        jnp.concatenate([cos_left, -sin_left], axis=1),
        jnp.concatenate([sin_left, cos_left], axis=1),
        jnp.concatenate([cos_right, -sin_right], axis=0),
        jnp.concatenate([sin_right, cos_right], axis=0),
    )


def cmul(a_real, a_imag, b_real, b_imag):
    return (a_real * b_real - a_imag * b_imag, a_real * b_imag + a_imag * b_real)


def cmul_conj(a_real, a_imag, b_real, b_imag):
    return (a_real * b_real + a_imag * b_imag, a_real * b_imag - a_imag * b_real)


def gather_slice(own, even, up):
    half = own.shape[1] // 2
    top, bottom = own[:, :half], own[:, half:]
    ahead_top = shift(top, -2)
    ahead_bottom = shift(bottom, -2)
    partner = swap(own)
    first = swap(ahead_top)
    far = hop(ahead_top, lambda i: i - 1 if i % 2 == 0 else None)
    behind_bottom, behind_top = up
    second = swap(jnp.where(even, ahead_bottom, behind_bottom))
    pick = lambda a, b: jnp.where(even, a, b)
    return {
        -3: behind_bottom,
        -2: pick(behind_top, partner[:, :half]),
        -1: pick(second, partner[:, half:]),
        0: top,
        1: bottom,
        2: pick(partner[:, :half], first),
        3: pick(partner[:, half:], second),
        4: ahead_top,
        5: ahead_bottom,
        6: pick(first, far),
    }


def window_of(pieces, edge, row, col):
    half = pieces[0].shape[1]
    place = lax.broadcasted_iota(jnp.int32, (1, half, 1), 1)
    low = jnp.where(place >= row, pieces[-3], pieces[5])
    high = jnp.where(place + half >= row, pieces[-2], pieces[6])
    rows = jnp.concatenate([low, high] + [pieces[j] for j in range(-1, 5)], axis=1)
    rest = rows.shape[2] - edge
    column = lax.broadcasted_iota(jnp.int32, (1, 1, rest), 2)
    start = jnp.where(column < col, rows[:, :, edge:], rows[:, :, :rest])
    return jnp.concatenate([start, rows[:, :, rest:edge]], axis=2)


def pieces_of(grad, half, cols, row, col):
    edge = grad.shape[1]
    rest = cols - edge
    column = lax.broadcasted_iota(jnp.int32, (1, 1, edge), 2)
    wide = jnp.concatenate(
        [
            jnp.where(column >= col, grad, 0.0),
            jnp.where(column[:, :, :rest] < col, grad[:, :, :rest], 0.0),
        ],
        axis=2,
    )
    block = [wide[:, q * half : (q + 1) * half] for q in range(edge // half)]
    place = lax.broadcasted_iota(jnp.int32, (1, half, 1), 1)
    out = {j: block[j + 3] for j in range(-1, 5)}
    out[-3] = jnp.where(place >= row, block[0], 0.0)
    out[5] = jnp.where(place >= row, 0.0, block[0])
    out[-2] = jnp.where(place + half >= row, block[1], 0.0)
    out[6] = jnp.where(place + half >= row, 0.0, block[1])
    return out


def scatter_slice(pieces, even):
    pick = lambda a, b: jnp.where(even, a, b)
    far = hop(pieces[6], lambda i: i + 1 if i % 2 == 1 else None)
    onward = swap(
        jnp.concatenate([pick(pieces[6], pieces[2]), pick(pieces[-1], pieces[3])], axis=1)
    )
    near = swap(
        jnp.concatenate([pick(pieces[2], pieces[-2]), pick(pieces[3], pieces[-1])], axis=1)
    )
    half = pieces[0].shape[1]
    from_behind_bottom = shift(pieces[5] + jnp.where(even, onward[:, half:], 0.0), 2)
    from_behind_top = shift(pieces[4] + onward[:, :half] + far, 2)
    from_ahead_bottom = shift(pieces[-3] + jnp.where(even, 0.0, onward[:, half:]), -2)
    from_ahead_top = hop(pieces[-2], lambda i: i - 1 if i % 2 == 0 else None)
    top = pieces[0] + near[:, :half] + from_behind_top + from_ahead_top
    bottom = pieces[1] + near[:, half:] + from_behind_bottom + from_ahead_bottom
    return jnp.concatenate([top, bottom], axis=1)


def body(object_field, row_offset, col_offset, amplitudes, probe, phase):
    strip, cols = object_field.shape[2:]
    half = strip // 2
    edge = probe.shape[1]
    row, col = row_offset[0], col_offset[0]
    even = lax.rem(lax.axis_index("row"), 2) == 0

    below = []
    for k in range(2):
        own = object_field[k]
        behind_bottom = shift(own[:, half:], 2)
        behind_top = hop(own[:, :half], lambda i: i + 1 if i % 2 == 1 else None)
        below.append((behind_bottom, behind_top))
    gathered = [gather_slice(object_field[k], even, below[k]) for k in range(2)]

    cos_base, sin_base = base_tables(edge)
    cos_rows, sin_rows = rolled(cos_base, row, 1), rolled(sin_base, row, 1)
    cos_cols, sin_cols = rolled(cos_base, col, 0), rolled(sin_base, col, 0)
    forward = transform_tables(cos_rows, sin_rows, cos_cols, sin_cols)
    inverse = transform_tables(cos_rows.T, -sin_rows.T, cos_cols.T, -sin_cols.T)
    prop_real, prop_imag = jnp.cos(phase), jnp.sin(phase)
    light = rolled(rolled(probe, row, 1), col, 2)

    first = window_of(gathered[0], edge, row, col)
    exit_real, exit_imag = cmul(light[0], light[1], first[0], first[1])
    freq_real, freq_imag = transform(exit_real, exit_imag, forward)
    moved_real, moved_imag = cmul(freq_real, freq_imag, prop_real, prop_imag)
    inner_real, inner_imag = transform(moved_real, moved_imag, inverse)

    second = window_of(gathered[1], edge, row, col)
    wave_real, wave_imag = cmul(inner_real, inner_imag, second[0], second[1])
    far_real, far_imag = transform(wave_real, wave_imag, forward)
    modulus = jnp.sqrt(far_real * far_real + far_imag * far_imag)
    ratio = amplitudes[0] / jnp.maximum(modulus, 0.1)
    resid_real = far_real * (1.0 - ratio)
    resid_imag = far_imag * (1.0 - ratio)
    back_real, back_imag = transform(resid_real, resid_imag, inverse)
    grad2 = jnp.stack(cmul_conj(inner_real, inner_imag, back_real, back_imag))
    total2 = scatter_slice(pieces_of(grad2, half, cols, row, col), even)

    mid_real, mid_imag = cmul_conj(second[0], second[1], back_real, back_imag)
    spec_real, spec_imag = transform(mid_real, mid_imag, forward)
    unprop_real, unprop_imag = cmul_conj(prop_real, prop_imag, spec_real, spec_imag)
    entry_real, entry_imag = transform(unprop_real, unprop_imag, inverse)
    grad1 = jnp.stack(cmul_conj(light[0], light[1], entry_real, entry_imag))
    total1 = scatter_slice(pieces_of(grad1, half, cols, row, col), even)
    return object_field - 0.5 * jnp.stack([total1, total2])


def solution(mesh):
    placed = (
        P(None, None, ("scan", "row"), None),
        P(("scan", "row")),
        P(("scan", "row")),
        P(("scan", "row"), None, None),
        P("scan", None, None),
        P(),
    )
    return jax.shard_map(
        body,
        mesh=mesh,
        in_specs=placed,
        out_specs=P(None, None, ("scan", "row"), None),
        check_vma=False,
    )
```

```python
import functools
import math

import jax
import jax.numpy as jnp
from jax import lax
from jax.experimental import pallas as pl
from jax.experimental.pallas import tpu as pltpu
from jax.sharding import PartitionSpec as P


def hop(block, route):
    size = lax.axis_size("row")
    pairs = [(i, route(i) % size) for i in range(size) if route(i) is not None]
    return lax.ppermute(block, "row", pairs)


def shift(block, distance):
    return hop(block, lambda i: i + distance)


def swap(block):
    return hop(block, lambda i: i ^ 1)


VMEM = pltpu.VMEM
ROWS_AT_ONCE = 128


def cmul(a_real, a_imag, b_real, b_imag):
    return (a_real * b_real - a_imag * b_imag, a_real * b_imag + a_imag * b_real)


def cmul_conj(a_real, a_imag, b_real, b_imag):
    return (a_real * b_real + a_imag * b_imag, a_real * b_imag - a_imag * b_real)


def wave_table(count, step, edge):
    index = lax.broadcasted_iota(jnp.int32, (count, edge), 0) * step
    across = lax.broadcasted_iota(jnp.int32, (count, edge), 1)
    angles = lax.rem(index * across, edge).astype(jnp.float32) * (-2.0 * math.pi / edge)
    return jnp.cos(angles), jnp.sin(angles)


def prepare_kernel(place, probe, left, left_back, right, right_back, light, cos_base, sin_base):
    edge = probe.shape[1]
    fine = 32
    row, col = place[0], place[1]
    factor = 1.0 / math.sqrt(edge)
    fine_cos, fine_sin = wave_table(fine, 1, edge)
    coarse_cos, coarse_sin = wave_table(edge // fine, fine, edge)
    for a in range(edge // fine):
        here = pl.ds(a * fine, fine)
        c, s = coarse_cos[a : a + 1], coarse_sin[a : a + 1]
        rounded = lambda x: (x * factor).astype(jnp.bfloat16).astype(jnp.float32)
        cos_base[here, :] = rounded(c * fine_cos - s * fine_sin)
        sin_base[here, :] = rounded(s * fine_cos + c * fine_sin)
    narrow = lambda x: x.astype(jnp.bfloat16)
    for part, base in enumerate((cos_base, sin_base)):
        here = pl.ds(part * edge, edge)
        left[part] = narrow(pltpu.roll(base[...], row, 1))
        left_back[part] = narrow(pltpu.roll(base[...], row, 0))
        right[here, :] = narrow(pltpu.roll(base[...], col, 0))
        right_back[here, :] = narrow(pltpu.roll(base[...], col, 1))
        light[part] = pltpu.roll(pltpu.roll(probe[part], row, 0), col, 1)


def whole(count):
    return [pl.BlockSpec(memory_space=VMEM)] * count


def prepare(place, probe):
    edge = probe.shape[1]
    pair = jax.ShapeDtypeStruct((2, edge, edge), jnp.bfloat16)
    tall = jax.ShapeDtypeStruct((2 * edge, edge), jnp.bfloat16)
    return pl.pallas_call(
        prepare_kernel,
        in_specs=[pl.BlockSpec(memory_space=pltpu.SMEM)] + whole(1),
        out_specs=whole(5),
        out_shape=[pair, pair, tall, tall, jax.ShapeDtypeStruct(probe.shape, jnp.float32)],
        scratch_shapes=[VMEM((edge, edge), jnp.float32)] * 2,
        compiler_params=pltpu.CompilerParams(vmem_limit_bytes=24 << 20),
        cost_estimate=pl.CostEstimate(flops=16 << 20, bytes_accessed=8 << 20, transcendentals=0),
        name="prepare",
    )(place, probe)


def spectrum(field, left, right, back, emit):
    edge = field.shape[1]
    count = ROWS_AT_ONCE

    @pl.loop(0, edge // count)
    def _(i):
        rows = pl.ds(pl.multiple_of(i * count, count), count)
        c, s = left[0, rows, :], left[1, rows, :]
        if back:
            lhs = [[c, s], [-s, c]]
        else:
            lhs = [[c, -s], [s, c]]
        join = lambda x: jnp.concatenate([jnp.concatenate(y, axis=1) for y in x], axis=0)
        both = jnp.dot(join(lhs), field[...], preferred_element_type=jnp.float32).astype(jnp.bfloat16)
        real, imag = both[:count], both[count:]
        if back:
            lhs = [[real, imag], [imag, -real]]
        else:
            lhs = [[real, -imag], [imag, real]]
        out = jnp.dot(join(lhs), right[...], preferred_element_type=jnp.float32)
        emit(rows, out[:count], out[count:])


def stacked_at(ref, rows):
    return pl.ds(pl.multiple_of(rows.start + ref.shape[1], ROWS_AT_ONCE), rows.size)


def put_field(ref, rows, real, imag):
    ref[rows, :] = real.astype(jnp.bfloat16)
    ref[stacked_at(ref, rows), :] = imag.astype(jnp.bfloat16)


def fill_window(place, own, partner, parts, mult, field, window):
    ahead_top, ahead_bottom, behind, first, second, far = parts
    edge = field.shape[1]
    half = ahead_top.shape[1]
    row, col, even = place[0], place[1], place[2] == 1
    rest = ahead_top.shape[2] - edge
    line = lax.broadcasted_iota(jnp.int32, (half, edge), 0)
    column = lax.broadcasted_iota(jnp.int32, (half, rest), 1)
    top, bottom = pl.ds(0, half), pl.ds(half, half)

    def at(ref, part, where):
        x = ref[part, where, :] if len(ref.shape) == 3 else ref[0, part, where, :]
        return jnp.concatenate(
            [jnp.where(column < col, x[:, edge:], x[:, :rest]), x[:, rest:edge]], axis=1
        )

    def rows_of(q, part):
        pick = lambda a, b: jnp.where(even, a, b)
        if q == 0:
            return jnp.where(line >= row, at(behind, part, bottom), at(ahead_bottom, part, top))
        if q == 1:
            low = pick(at(second, part, top), at(partner, part, top))
            high = pick(at(first, part, top), far[part])
            return jnp.where(line + half >= row, low, high)
        if q == 2:
            return pick(at(second, part, bottom), at(partner, part, bottom))
        if q == 3:
            return at(own, part, top)
        if q == 4:
            return at(own, part, bottom)
        if q == 5:
            return pick(at(partner, part, top), at(first, part, top))
        if q == 6:
            return pick(at(partner, part, bottom), at(second, part, top))
        return at(ahead_top, part, top)

    for q in range(edge // half):
        here = pl.ds(q * half, half)
        real, imag = rows_of(q, 0), rows_of(q, 1)
        if window is not None:
            window[0, here, :] = real
            window[1, here, :] = imag
        out_real, out_imag = cmul(mult[0, here, :], mult[1, here, :], real, imag)
        field[here, :] = out_real.astype(jnp.bfloat16)
        field[pl.ds(edge + q * half, half), :] = out_imag.astype(jnp.bfloat16)


def put_pieces(place, mult, back, send, relay, keep):
    edge = back.shape[1]
    half = relay.shape[1]
    rest = keep.shape[2] - edge
    row, col, even = place[0], place[1], place[2] == 1
    line = lax.broadcasted_iota(jnp.int32, (half, edge), 0)
    column = lax.broadcasted_iota(jnp.int32, (half, edge), 1)
    left, right = pl.ds(0, edge), pl.ds(edge, rest)

    def put(ref, slot, part, value):
        at = pl.ds(slot * half, half) if isinstance(slot, int) else pl.ds(pl.multiple_of(slot * half, half), half)
        ref[part, at, left] = jnp.where(column >= col, value, 0.0)
        ref[part, at, right] = jnp.where(column[:, :rest] < col, value[:, :rest], 0.0)

    by = lambda a, b: jnp.where(even, a, b)
    for q in range(edge // half):
        here = pl.ds(q * half, half)
        grad = cmul_conj(mult[0, here, :], mult[1, here, :], back[0, here, :], back[1, here, :])
        for part, value in enumerate(grad):
            if q == 0:
                put(keep, 4, part, jnp.where(line >= row, value, 0.0))
                put(keep, 3, part, jnp.where(line >= row, 0.0, value))
            elif q == 1:
                high = jnp.where(line + half >= row, 0.0, value)
                relay[part, :, :] = high
                put(send, by(4, 0), part, jnp.where(line + half >= row, value, 0.0))
                put(send, by(2, 4), part, high)
            elif q in (2, 5, 6):
                put(send, {2: by(3, 1), 5: by(0, 2), 6: by(1, 3)}[q], part, value)
            else:
                put(keep, {3: 0, 4: 1, 7: 2}[q], part, value)


def inward_kernel(place, own, partner, a, b, c, d, e, f, light, turn, left, left_back, right, right_back, inner, field, moved):
    fill_window(place, own, partner, (a, b, c, d, e, f), light, field, None)

    def propagate(rows, real, imag):
        put_field(moved, rows, *cmul(real, imag, turn[0, rows, :], turn[1, rows, :]))

    spectrum(field, left, right, False, propagate)

    def store(rows, real, imag):
        inner[0, rows, :] = real
        inner[1, rows, :] = imag

    spectrum(moved, left_back, right_back, True, store)


def turn_kernel(place, own, partner, a, b, c, d, e, f, inner, amplitude, left, left_back, right, right_back, send, relay, keep, mid, field, moved, window, back):
    fill_window(place, own, partner, (a, b, c, d, e, f), inner, field, window)

    def residual(rows, real, imag):
        modulus = jnp.sqrt(real * real + imag * imag)
        scale = 1.0 - amplitude[0, rows, :] / jnp.maximum(modulus, 0.1)
        put_field(moved, rows, real * scale, imag * scale)

    spectrum(field, left, right, False, residual)

    def store(rows, real, imag):
        back[0, rows, :] = real
        back[1, rows, :] = imag
        put_field(mid, rows, *cmul_conj(window[0, rows, :], window[1, rows, :], real, imag))

    spectrum(moved, left_back, right_back, True, store)
    put_pieces(place, inner, back, send, relay, keep)


def outward_kernel(place, mid, light, turn, left, left_back, right, right_back, send, relay, keep, moved, back):
    def propagate(rows, real, imag):
        put_field(moved, rows, *cmul_conj(turn[0, rows, :], turn[1, rows, :], real, imag))

    spectrum(mid, left, right, False, propagate)

    def store(rows, real, imag):
        back[0, rows, :] = real
        back[1, rows, :] = imag

    spectrum(moved, left_back, right_back, True, store)
    put_pieces(place, light, back, send, relay, keep)


def run(kernel, in_specs, arguments, out_shape, scratch):
    return pl.pallas_call(
        kernel,
        grid=(1,),
        in_specs=in_specs,
        out_specs=[pl.BlockSpec(x.shape, functools.partial(lambda n, i: (0,) * n, len(x.shape))) for x in out_shape],
        out_shape=out_shape,
        scratch_shapes=scratch,
        compiler_params=pltpu.CompilerParams(vmem_limit_bytes=36 << 20),
        cost_estimate=pl.CostEstimate(flops=4 << 30, bytes_accessed=16 << 20, transcendentals=0),
    )(*arguments)


def full(x):
    return pl.BlockSpec(x.shape, lambda i: (0,) * x.ndim)


def strip_of(k, x):
    return pl.BlockSpec((1,) + x.shape[1:], lambda i: (k, 0, 0, 0))


def piece_shapes(half, edge, cols):
    wide = jax.ShapeDtypeStruct((2, 5 * half, cols), jnp.float32)
    return [wide, jax.ShapeDtypeStruct((2, half, edge), jnp.float32), wide]


def after(value, *others):
    return lax.optimization_barrier((value,) + others)[0]


def widened(x, start, cols):
    edge = x.shape[2]
    column = lax.broadcasted_iota(jnp.int32, (1, 1, edge), 2)
    rest = cols - edge
    return jnp.concatenate(
        [
            jnp.where(column >= start, x, 0.0),
            jnp.where(column[:, :, :rest] < start, x[:, :, :rest], 0.0),
        ],
        axis=2,
    )


def narrowed(x, start, edge):
    rest = x.shape[2] - edge
    column = lax.broadcasted_iota(jnp.int32, (1, 1, rest), 2)
    return jnp.concatenate(
        [jnp.where(column < start, x[:, :, edge:], x[:, :, :rest]), x[:, :, rest:edge]], axis=2
    )


def scattered(send, relay, keep, even, far_col, then):
    half = relay.shape[1]
    block = lambda x, slot: x[:, slot * half : (slot + 1) * half]
    far = hop(relay, lambda i: i + 1 if i % 2 == 1 else None)
    got = swap(send)
    to_bottom = block(keep, 3) + jnp.where(even, block(got, 3), 0.0)
    to_back = jnp.concatenate(
        [
            jnp.where(even, 0.0, block(got, 4)),
            block(keep, 4) + jnp.where(even, 0.0, block(got, 3)),
        ],
        axis=1,
    )
    far = after(far, to_bottom, to_back)
    to_top = block(keep, 2) + block(got, 2) + widened(far, far_col, keep.shape[2])
    if then is not None:
        to_top, then = lax.optimization_barrier((to_top, then))
    bottom, ahead = shift(to_bottom, 2), shift(to_back, -2)
    top = shift(to_top, 2)
    mine = keep[:, : 2 * half] + got[:, : 2 * half]
    return (mine, ahead, top, bottom), then


def total_of(parts):
    mine, ahead, top, bottom = parts
    return mine + ahead + jnp.concatenate([top, bottom], axis=1)


def body(object_field, row_offset, col_offset, amplitudes, probe, phase):
    strip, cols = object_field.shape[2:]
    half = strip // 2
    edge = probe.shape[1]
    even = lax.rem(lax.axis_index("row"), 2) == 0
    place = jnp.stack([row_offset[0], col_offset[0], even.astype(jnp.int32)])

    lead = lax.optimization_barrier(object_field[0, :, :half])
    rest_field = after(object_field, lead)
    far_col = shift(col_offset, 1)[0]
    top0 = shift(lead, -2)
    bottom0 = shift(rest_field[0, :, half:], -2)
    behind0 = shift(rest_field[0], 2)
    partner = swap(rest_field)
    left, left_back, right, right_back, light = prepare(place, probe)

    carried = lax.optimization_barrier(narrowed(top0, far_col, edge))
    far0 = hop(carried, lambda i: i - 1 if i % 2 == 0 else None)
    first0 = swap(top0)
    later_field, phase = lax.optimization_barrier((rest_field, phase, carried))[:2]
    top1 = shift(later_field[1, :, :half], -2)
    behind1 = shift(after(later_field, bottom0)[1], 2)
    turn = jnp.stack([jnp.cos(phase), jnp.sin(phase)])
    crossing = jnp.where(even, jnp.concatenate([bottom0, bottom0], axis=1), behind0)
    crossing = lax.optimization_barrier(crossing)
    second0 = swap(crossing)
    bottom1 = shift(after(later_field, crossing)[1, :, half:], -2)

    first1 = swap(top1)
    far_col_later, even_later = lax.optimization_barrier((far_col, even, far0, second0))[:2]
    carried = narrowed(top1, far_col_later, edge)
    far1 = hop(carried, lambda i: i - 1 if i % 2 == 0 else None)
    crossing = jnp.where(even_later, jnp.concatenate([bottom1, bottom1], axis=1), behind1)
    second1 = swap(crossing)

    waves = (left, left_back, right, right_back)
    smem = pl.BlockSpec(memory_space=pltpu.SMEM)
    square = jax.ShapeDtypeStruct((2, edge, edge), jnp.float32)
    field = jax.ShapeDtypeStruct((2 * edge, edge), jnp.bfloat16)
    scratch = [VMEM(x.shape, x.dtype) for x in (field, field, square, square)]

    parts = (top0, bottom0, behind0, first0, second0, far0)
    arguments = parts + (light, turn) + waves
    (inner,) = run(
        inward_kernel,
        [smem, strip_of(0, object_field), strip_of(0, partner)] + [full(x) for x in arguments],
        (place, object_field, partner) + arguments,
        [square],
        scratch[:2],
    )

    parts = (top1, bottom1, behind1, first1, second1, far1)
    arguments = parts + (inner, amplitudes) + waves
    send, relay, keep, mid = run(
        turn_kernel,
        [smem, strip_of(1, object_field), strip_of(1, partner)] + [full(x) for x in arguments],
        (place, object_field, partner) + arguments,
        piece_shapes(half, edge, cols) + [field],
        scratch,
    )
    shares2, mid = scattered(send, relay, keep, even, far_col, mid)

    arguments = (mid, light, turn) + waves
    send, relay, keep = run(
        outward_kernel,
        [smem] + [full(x) for x in arguments],
        (place,) + arguments,
        piece_shapes(half, edge, cols),
        [scratch[0], scratch[2]],
    )
    shares1, _ = scattered(send, relay, keep, even, far_col, None)
    return object_field - 0.5 * jnp.stack([total_of(shares1), total_of(shares2)])


def solution(mesh):
    placed = (
        P(None, None, ("scan", "row"), None),
        P(("scan", "row")),
        P(("scan", "row")),
        P(("scan", "row"), None, None),
        P("scan", None, None),
        P(),
    )
    return jax.shard_map(
        body,
        mesh=mesh,
        in_specs=placed,
        out_specs=P(None, None, ("scan", "row"), None),
        check_vma=False,
    )
```

```python
import functools
import math

import jax
import jax.numpy as jnp
from jax import lax
from jax.experimental import pallas as pl
from jax.experimental.pallas import tpu as pltpu
from jax.sharding import PartitionSpec as P


def hop(block, route):
    size = lax.axis_size("row")
    pairs = [(i, route(i) % size) for i in range(size) if route(i) is not None]
    return lax.ppermute(block, "row", pairs)


def shift(block, distance):
    return hop(block, lambda i: i + distance)


def swap(block):
    return hop(block, lambda i: i ^ 1)


VMEM = pltpu.VMEM
ROWS_AT_ONCE = 128


def cmul(a_real, a_imag, b_real, b_imag):
    return (a_real * b_real - a_imag * b_imag, a_real * b_imag + a_imag * b_real)


def cmul_conj(a_real, a_imag, b_real, b_imag):
    return (a_real * b_real + a_imag * b_imag, a_real * b_imag - a_imag * b_real)


def wave_table(count, step, edge):
    index = lax.broadcasted_iota(jnp.int32, (count, edge), 0) * step
    across = lax.broadcasted_iota(jnp.int32, (count, edge), 1)
    angles = lax.rem(index * across, edge).astype(jnp.float32) * (-2.0 * math.pi / edge)
    return jnp.cos(angles), jnp.sin(angles)


def prepare_kernel(place, probe, left, left_back, right, right_back, light, cos_base, sin_base):
    edge = probe.shape[1]
    fine = 32
    row, col = place[0], place[1]
    factor = 1.0 / math.sqrt(edge)
    fine_cos, fine_sin = wave_table(fine, 1, edge)
    coarse_cos, coarse_sin = wave_table(edge // fine, fine, edge)
    for a in range(edge // fine):
        here = pl.ds(a * fine, fine)
        c, s = coarse_cos[a : a + 1], coarse_sin[a : a + 1]
        rounded = lambda x: (x * factor).astype(jnp.bfloat16).astype(jnp.float32)
        cos_base[here, :] = rounded(c * fine_cos - s * fine_sin)
        sin_base[here, :] = rounded(s * fine_cos + c * fine_sin)
    narrow = lambda x: x.astype(jnp.bfloat16)
    for part, base in enumerate((cos_base, sin_base)):
        here = pl.ds(part * edge, edge)
        left[part] = narrow(pltpu.roll(base[...], row, 1))
        left_back[part] = narrow(pltpu.roll(base[...], row, 0))
        right[here, :] = narrow(pltpu.roll(base[...], col, 0))
        right_back[here, :] = narrow(pltpu.roll(base[...], col, 1))
        light[part] = pltpu.roll(pltpu.roll(probe[part], row, 0), col, 1)


def whole(count):
    return [pl.BlockSpec(memory_space=VMEM)] * count


def prepare(place, probe):
    edge = probe.shape[1]
    pair = jax.ShapeDtypeStruct((2, edge, edge), jnp.bfloat16)
    tall = jax.ShapeDtypeStruct((2 * edge, edge), jnp.bfloat16)
    return pl.pallas_call(
        prepare_kernel,
        in_specs=[pl.BlockSpec(memory_space=pltpu.SMEM)] + whole(1),
        out_specs=whole(5),
        out_shape=[pair, pair, tall, tall, jax.ShapeDtypeStruct(probe.shape, jnp.float32)],
        scratch_shapes=[VMEM((edge, edge), jnp.float32)] * 2,
        compiler_params=pltpu.CompilerParams(vmem_limit_bytes=16 << 20),
        cost_estimate=pl.CostEstimate(flops=16 << 20, bytes_accessed=8 << 20, transcendentals=0),
        name="prepare",
    )(place, probe)


def spectrum(field, left, right, back, emit):
    edge = field.shape[1]
    count = ROWS_AT_ONCE

    @pl.loop(0, edge // count)
    def _(i):
        rows = pl.ds(pl.multiple_of(i * count, count), count)
        c, s = left[0, rows, :], left[1, rows, :]
        if back:
            lhs = [[c, s], [-s, c]]
        else:
            lhs = [[c, -s], [s, c]]
        join = lambda x: jnp.concatenate([jnp.concatenate(y, axis=1) for y in x], axis=0)
        both = jnp.dot(join(lhs), field[...], preferred_element_type=jnp.float32).astype(jnp.bfloat16)
        real, imag = both[:count], both[count:]
        if back:
            lhs = [[real, imag], [imag, -real]]
        else:
            lhs = [[real, -imag], [imag, real]]
        out = jnp.dot(join(lhs), right[...], preferred_element_type=jnp.float32)
        emit(rows, out[:count], out[count:])


def stacked_at(ref, rows):
    return pl.ds(pl.multiple_of(rows.start + ref.shape[1], ROWS_AT_ONCE), rows.size)


def put_field(ref, rows, real, imag):
    ref[rows, :] = real.astype(jnp.bfloat16)
    ref[stacked_at(ref, rows), :] = imag.astype(jnp.bfloat16)


def fill_window(place, own, partner, parts, mult, field, window):
    ahead_top, ahead_bottom, behind, first, second, far = parts
    edge = field.shape[1]
    half = ahead_top.shape[1]
    row, col, even = place[0], place[1], place[2] == 1
    rest = ahead_top.shape[2] - edge
    line = lax.broadcasted_iota(jnp.int32, (half, edge), 0)
    column = lax.broadcasted_iota(jnp.int32, (half, rest), 1)
    top, bottom = pl.ds(0, half), pl.ds(half, half)

    def at(ref, part, where):
        x = ref[part, where, :] if len(ref.shape) == 3 else ref[0, part, where, :]
        return jnp.concatenate(
            [jnp.where(column < col, x[:, edge:], x[:, :rest]), x[:, rest:edge]], axis=1
        )

    def rows_of(q, part):
        pick = lambda a, b: jnp.where(even, a, b)
        if q == 0:
            return jnp.where(line >= row, at(behind, part, bottom), at(ahead_bottom, part, top))
        if q == 1:
            low = pick(at(second, part, top), at(partner, part, top))
            high = pick(at(first, part, top), far[part])
            return jnp.where(line + half >= row, low, high)
        if q == 2:
            return pick(at(second, part, bottom), at(partner, part, bottom))
        if q == 3:
            return at(own, part, top)
        if q == 4:
            return at(own, part, bottom)
        if q == 5:
            return pick(at(partner, part, top), at(first, part, top))
        if q == 6:
            return pick(at(partner, part, bottom), at(second, part, top))
        return at(ahead_top, part, top)

    for q in range(edge // half):
        here = pl.ds(q * half, half)
        real, imag = rows_of(q, 0), rows_of(q, 1)
        if window is not None:
            window[0, here, :] = real
            window[1, here, :] = imag
        out_real, out_imag = cmul(mult[0, here, :], mult[1, here, :], real, imag)
        field[here, :] = out_real.astype(jnp.bfloat16)
        field[pl.ds(edge + q * half, half), :] = out_imag.astype(jnp.bfloat16)


def put_pieces(place, mult, back, send, relay, early, keep):
    edge = back.shape[1]
    half = relay.shape[1]
    rest = keep.shape[2] - edge
    row, col, even = place[0], place[1], place[2] == 1
    line = lax.broadcasted_iota(jnp.int32, (half, edge), 0)
    column = lax.broadcasted_iota(jnp.int32, (half, edge), 1)
    left, right = pl.ds(0, edge), pl.ds(edge, rest)

    def put(ref, slot, part, value):
        at = pl.ds(slot * half, half) if isinstance(slot, int) else pl.ds(pl.multiple_of(slot * half, half), half)
        ref[part, at, left] = jnp.where(column >= col, value, 0.0)
        ref[part, at, right] = jnp.where(column[:, :rest] < col, value[:, :rest], 0.0)

    by = lambda a, b: jnp.where(even, a, b)
    for q in range(edge // half):
        here = pl.ds(q * half, half)
        grad = cmul_conj(mult[0, here, :], mult[1, here, :], back[0, here, :], back[1, here, :])
        for part, value in enumerate(grad):
            if q == 0:
                put(keep, 4, part, jnp.where(line >= row, value, 0.0))
                high = jnp.where(line >= row, 0.0, value)
                put(keep, 3, part, high)
                early[part, :, :] = high
            elif q == 1:
                high = jnp.where(line + half >= row, 0.0, value)
                relay[part, :, :] = high
                put(send, by(4, 0), part, jnp.where(line + half >= row, value, 0.0))
                put(send, by(2, 4), part, high)
            elif q in (2, 5, 6):
                put(send, {2: by(3, 1), 5: by(0, 2), 6: by(1, 3)}[q], part, value)
            else:
                put(keep, {3: 0, 4: 1, 7: 2}[q], part, value)


def inward_kernel(place, own, partner, a, b, c, d, e, f, light, turn, left, left_back, right, right_back, inner, field, moved):
    fill_window(place, own, partner, (a, b, c, d, e, f), light, field, None)

    def propagate(rows, real, imag):
        put_field(moved, rows, *cmul(real, imag, turn[0, rows, :], turn[1, rows, :]))

    spectrum(field, left, right, False, propagate)

    def store(rows, real, imag):
        inner[0, rows, :] = real
        inner[1, rows, :] = imag

    spectrum(moved, left_back, right_back, True, store)


def turn_kernel(place, own, partner, a, b, c, d, e, f, inner, amplitude, left, left_back, right, right_back, send, relay, early, keep, mid, field, moved, window, back):
    fill_window(place, own, partner, (a, b, c, d, e, f), inner, field, window)

    def residual(rows, real, imag):
        modulus = jnp.sqrt(real * real + imag * imag)
        scale = 1.0 - amplitude[0, rows, :] / jnp.maximum(modulus, 0.1)
        put_field(moved, rows, real * scale, imag * scale)

    spectrum(field, left, right, False, residual)

    def store(rows, real, imag):
        back[0, rows, :] = real
        back[1, rows, :] = imag
        put_field(mid, rows, *cmul_conj(window[0, rows, :], window[1, rows, :], real, imag))

    spectrum(moved, left_back, right_back, True, store)
    put_pieces(place, inner, back, send, relay, early, keep)


def outward_kernel(place, mid, light, turn, left, left_back, right, right_back, send, relay, early, keep, moved, back):
    def propagate(rows, real, imag):
        put_field(moved, rows, *cmul_conj(turn[0, rows, :], turn[1, rows, :], real, imag))

    spectrum(mid, left, right, False, propagate)

    def store(rows, real, imag):
        back[0, rows, :] = real
        back[1, rows, :] = imag

    spectrum(moved, left_back, right_back, True, store)
    put_pieces(place, light, back, send, relay, early, keep)


def run(kernel, in_specs, arguments, out_shape, scratch):
    return pl.pallas_call(
        kernel,
        grid=(1,),
        in_specs=in_specs,
        out_specs=[pl.BlockSpec(x.shape, functools.partial(lambda n, i: (0,) * n, len(x.shape))) for x in out_shape],
        out_shape=out_shape,
        scratch_shapes=scratch,
        compiler_params=pltpu.CompilerParams(vmem_limit_bytes=16 << 20),
        cost_estimate=pl.CostEstimate(flops=4 << 30, bytes_accessed=16 << 20, transcendentals=0),
    )(*arguments)


def full(x):
    return pl.BlockSpec(x.shape, lambda i: (0,) * x.ndim)


def strip_of(k, x):
    return pl.BlockSpec((1,) + x.shape[1:], lambda i: (k, 0, 0, 0))


def piece_shapes(half, edge, cols):
    wide = jax.ShapeDtypeStruct((2, 5 * half, cols), jnp.float32)
    narrow = jax.ShapeDtypeStruct((2, half, edge), jnp.float32)
    return [wide, narrow, narrow, wide]


def after(value, *others):
    return lax.optimization_barrier((value,) + others)[0]


def widened(x, start, cols):
    edge = x.shape[2]
    rest = cols - edge
    column = lax.broadcasted_iota(jnp.int32, x.shape, 2)
    kept = jnp.where(column >= start, x, 0.0)
    wrapped = jnp.where(column < start, x, 0.0)[:, :, :rest]
    return jnp.concatenate([kept, wrapped], axis=2)


def narrowed(x, start, edge):
    rest = x.shape[2] - edge
    column = lax.broadcasted_iota(jnp.int32, x.shape[:2] + (rest,), 2)
    return jnp.concatenate(
        [jnp.where(column < start, x[:, :, edge:], x[:, :, :rest]), x[:, :, rest:edge]], axis=2
    )


def scattered(send, relay, early, keep, even, far_col, then):
    half = relay.shape[1]
    cols = keep.shape[2]
    block = lambda x, slot: x[:, slot * half : (slot + 1) * half]
    far = hop(relay, lambda i: i + 1 if i % 2 == 1 else None)
    early = hop(early, lambda i: i + 2 if i % 2 == 1 else None)
    got = swap(send)
    to_bottom = block(keep, 3) + block(got, 3)
    to_back = jnp.concatenate(
        [
            jnp.where(even, 0.0, block(got, 4)),
            block(keep, 4) + jnp.where(even, 0.0, block(got, 3)),
        ],
        axis=1,
    )
    far = after(far, to_bottom, to_back)
    to_top = block(keep, 2) + block(got, 2) + widened(far, far_col, cols)
    if then is not None:
        to_top, then = lax.optimization_barrier((to_top, then))
    late = hop(to_bottom, lambda i: i + 2 if i % 2 == 0 else None)
    top, ahead = shift(to_top, 2), shift(to_back, -2)
    mine = keep[:, : 2 * half] + got[:, : 2 * half]
    return (mine, ahead, top, late, early), then


def total_of(parts, beyond):
    mine, ahead, top, late, early = parts
    bottom = late + widened(early, beyond, mine.shape[2])
    return mine + ahead + jnp.concatenate([top, bottom], axis=1)


def body(object_field, row_offset, col_offset, amplitudes, probe, phase):
    strip, cols = object_field.shape[2:]
    half = strip // 2
    edge = probe.shape[1]
    even = lax.rem(lax.axis_index("row"), 2) == 0
    place = jnp.stack([row_offset[0], col_offset[0], even.astype(jnp.int32)])

    lead = lax.optimization_barrier(object_field[0, :, :half])
    rest_field = after(object_field, lead)
    top0 = shift(lead, -2)
    far_col = hop(col_offset, lambda i: i + 1 if i % 2 == 1 else None)[0]
    bottom0 = shift(rest_field[0, :, half:], -2)
    behind0 = shift(rest_field[0], 2)
    partner = swap(rest_field)
    turn = jnp.stack([jnp.cos(phase), jnp.sin(phase)])

    carried = lax.optimization_barrier(narrowed(top0, far_col, edge))
    far0 = hop(carried, lambda i: i - 1 if i % 2 == 0 else None)
    first0 = swap(top0)
    later_field = after(rest_field, carried)
    top1 = shift(later_field[1, :, :half], -2)
    bottom1 = shift(later_field[1, :, half:], -2)
    behind1 = shift(later_field[1], 2)
    beyond = hop(col_offset, lambda i: i + 2 if i % 2 == 1 else None)[0]
    left, left_back, right, right_back, light = prepare(place, probe)

    even_after = after(even, light)
    crossing = jnp.where(even_after, jnp.concatenate([bottom0, bottom0], axis=1), behind0)
    second0 = swap(crossing)

    waves = (left, left_back, right, right_back)
    smem = pl.BlockSpec(memory_space=pltpu.SMEM)
    square = jax.ShapeDtypeStruct((2, edge, edge), jnp.float32)
    field = jax.ShapeDtypeStruct((2 * edge, edge), jnp.bfloat16)
    scratch = [VMEM(x.shape, x.dtype) for x in (field, field, square, square)]

    parts = (top0, bottom0, behind0, first0, second0, far0)
    arguments = parts + (light, turn) + waves
    (inner,) = run(
        inward_kernel,
        [smem, strip_of(0, object_field), strip_of(0, partner)] + [full(x) for x in arguments],
        (place, object_field, partner) + arguments,
        [square],
        scratch[:2],
    )

    top1_after, even_after = lax.optimization_barrier((top1, even, inner))[:2]
    carried = narrowed(top1_after, far_col, edge)
    far1 = hop(carried, lambda i: i - 1 if i % 2 == 0 else None)
    first1 = swap(top1_after)
    crossing = jnp.where(even_after, jnp.concatenate([bottom1, bottom1], axis=1), behind1)
    second1 = swap(crossing)

    parts = (top1, bottom1, behind1, first1, second1, far1)
    arguments = parts + (inner, amplitudes) + waves
    send, relay, early, keep, mid = run(
        turn_kernel,
        [smem, strip_of(1, object_field), strip_of(1, partner)] + [full(x) for x in arguments],
        (place, object_field, partner) + arguments,
        piece_shapes(half, edge, cols) + [field],
        scratch,
    )
    shares2, mid = scattered(send, relay, early, keep, even, far_col, mid)

    arguments = (mid, light, turn) + waves
    send, relay, early, keep = run(
        outward_kernel,
        [smem] + [full(x) for x in arguments],
        (place,) + arguments,
        piece_shapes(half, edge, cols),
        [scratch[0], scratch[2]],
    )
    shares1, _ = scattered(send, relay, early, keep, even, far_col, None)
    return object_field - 0.5 * jnp.stack(
        [total_of(shares1, beyond), total_of(shares2, beyond)]
    )


def solution(mesh):
    placed = (
        P(None, None, ("scan", "row"), None),
        P(("scan", "row")),
        P(("scan", "row")),
        P(("scan", "row"), None, None),
        P("scan", None, None),
        P(),
    )
    return jax.shard_map(
        body,
        mesh=mesh,
        in_specs=placed,
        out_specs=P(None, None, ("scan", "row"), None),
        check_vma=False,
    )
```

```python
import functools
import math

import jax
import jax.numpy as jnp
from jax import lax
from jax.experimental import pallas as pl
from jax.experimental.pallas import tpu as pltpu
from jax.sharding import PartitionSpec as P


def hop(block, route):
    size = lax.axis_size("row")
    pairs = [(i, route(i) % size) for i in range(size) if route(i) is not None]
    return lax.ppermute(block, "row", pairs)


def shift(block, distance):
    return hop(block, lambda i: i + distance)


def swap(block):
    return hop(block, lambda i: i ^ 1)


VMEM = pltpu.VMEM
ROWS_AT_ONCE = 128


def cmul(a_real, a_imag, b_real, b_imag):
    return (a_real * b_real - a_imag * b_imag, a_real * b_imag + a_imag * b_real)


def cmul_conj(a_real, a_imag, b_real, b_imag):
    return (a_real * b_real + a_imag * b_imag, a_real * b_imag - a_imag * b_real)


def wave_table(count, step, edge):
    index = lax.broadcasted_iota(jnp.int32, (count, edge), 0) * step
    across = lax.broadcasted_iota(jnp.int32, (count, edge), 1)
    angles = lax.rem(index * across, edge).astype(jnp.float32) * (-2.0 * math.pi / edge)
    return jnp.cos(angles), jnp.sin(angles)


def prepare_kernel(place, probe, left, left_back, right, right_back, light, cos_base, sin_base):
    edge = probe.shape[1]
    fine = 32
    row, col = place[0], place[1]
    factor = 1.0 / math.sqrt(edge)
    fine_cos, fine_sin = wave_table(fine, 1, edge)
    coarse_cos, coarse_sin = wave_table(edge // fine, fine, edge)
    for a in range(edge // fine):
        here = pl.ds(a * fine, fine)
        c, s = coarse_cos[a : a + 1], coarse_sin[a : a + 1]
        rounded = lambda x: (x * factor).astype(jnp.bfloat16).astype(jnp.float32)
        cos_base[here, :] = rounded(c * fine_cos - s * fine_sin)
        sin_base[here, :] = rounded(s * fine_cos + c * fine_sin)
    narrow = lambda x: x.astype(jnp.bfloat16)
    for part, base in enumerate((cos_base, sin_base)):
        here = pl.ds(part * edge, edge)
        left[part] = narrow(pltpu.roll(base[...], row, 1))
        left_back[part] = narrow(pltpu.roll(base[...], row, 0))
        right[here, :] = narrow(pltpu.roll(base[...], col, 0))
        right_back[here, :] = narrow(pltpu.roll(base[...], col, 1))
        light[part] = pltpu.roll(pltpu.roll(probe[part], row, 0), col, 1)


def whole(count):
    return [pl.BlockSpec(memory_space=VMEM)] * count


def prepare(place, probe):
    edge = probe.shape[1]
    pair = jax.ShapeDtypeStruct((2, edge, edge), jnp.bfloat16)
    tall = jax.ShapeDtypeStruct((2 * edge, edge), jnp.bfloat16)
    return pl.pallas_call(
        prepare_kernel,
        in_specs=[pl.BlockSpec(memory_space=pltpu.SMEM)] + whole(1),
        out_specs=whole(5),
        out_shape=[pair, pair, tall, tall, jax.ShapeDtypeStruct(probe.shape, jnp.float32)],
        scratch_shapes=[VMEM((edge, edge), jnp.float32)] * 2,
        compiler_params=pltpu.CompilerParams(vmem_limit_bytes=16 << 20),
        cost_estimate=pl.CostEstimate(flops=16 << 20, bytes_accessed=8 << 20, transcendentals=0),
        name="prepare",
    )(place, probe)


def spectrum(field, left, right, back, emit):
    edge = field.shape[1]
    count = ROWS_AT_ONCE

    @pl.loop(0, edge // count)
    def _(i):
        rows = pl.ds(pl.multiple_of(i * count, count), count)
        c, s = left[0, rows, :], left[1, rows, :]
        if back:
            lhs = [[c, s], [-s, c]]
        else:
            lhs = [[c, -s], [s, c]]
        join = lambda x: jnp.concatenate([jnp.concatenate(y, axis=1) for y in x], axis=0)
        both = jnp.dot(join(lhs), field[...], preferred_element_type=jnp.float32).astype(jnp.bfloat16)
        real, imag = both[:count], both[count:]
        if back:
            lhs = [[real, imag], [imag, -real]]
        else:
            lhs = [[real, -imag], [imag, real]]
        out = jnp.dot(join(lhs), right[...], preferred_element_type=jnp.float32)
        emit(rows, out[:count], out[count:])


def stacked_at(ref, rows):
    return pl.ds(pl.multiple_of(rows.start + ref.shape[1], ROWS_AT_ONCE), rows.size)


def put_field(ref, rows, real, imag):
    ref[rows, :] = real.astype(jnp.bfloat16)
    ref[stacked_at(ref, rows), :] = imag.astype(jnp.bfloat16)


def fill_window(place, own, partner, parts, mult, field, window):
    ahead_top, ahead_bottom, behind, swapped, far = parts
    edge = field.shape[1]
    half = far.shape[1]
    if ahead_bottom is None:
        ahead_top, ahead_bottom = (ahead_top.at[:, pl.ds(i * half, half), :] for i in range(2))
    first, second = swapped.at[:, pl.ds(0, half), :], swapped.at[:, pl.ds(half, 2 * half), :]
    row, col, even = place[0], place[1], place[2] == 1
    rest = ahead_top.shape[2] - edge
    line = lax.broadcasted_iota(jnp.int32, (half, edge), 0)
    column = lax.broadcasted_iota(jnp.int32, (half, rest), 1)
    top, bottom = pl.ds(0, half), pl.ds(half, half)

    def at(ref, part, where):
        x = ref[part, where, :] if len(ref.shape) == 3 else ref[0, part, where, :]
        return jnp.concatenate(
            [jnp.where(column < col, x[:, edge:], x[:, :rest]), x[:, rest:edge]], axis=1
        )

    def rows_of(q, part):
        pick = lambda a, b: jnp.where(even, a, b)
        if q == 0:
            return jnp.where(line >= row, at(behind, part, bottom), at(ahead_bottom, part, top))
        if q == 1:
            low = pick(at(second, part, top), at(partner, part, top))
            high = pick(at(first, part, top), far[part])
            return jnp.where(line + half >= row, low, high)
        if q == 2:
            return pick(at(second, part, bottom), at(partner, part, bottom))
        if q == 3:
            return at(own, part, top)
        if q == 4:
            return at(own, part, bottom)
        if q == 5:
            return pick(at(partner, part, top), at(first, part, top))
        if q == 6:
            return pick(at(partner, part, bottom), at(second, part, top))
        return at(ahead_top, part, top)

    for q in range(edge // half):
        here = pl.ds(q * half, half)
        real, imag = rows_of(q, 0), rows_of(q, 1)
        if window is not None:
            window[0, here, :] = real
            window[1, here, :] = imag
        out_real, out_imag = cmul(mult[0, here, :], mult[1, here, :], real, imag)
        field[here, :] = out_real.astype(jnp.bfloat16)
        field[pl.ds(edge + q * half, half), :] = out_imag.astype(jnp.bfloat16)


def put_pieces(place, mult, back, send, relay, keep):
    edge = back.shape[1]
    half = relay.shape[1]
    rest = keep.shape[2] - edge
    row, col, even = place[0], place[1], place[2] == 1
    line = lax.broadcasted_iota(jnp.int32, (half, edge), 0)
    column = lax.broadcasted_iota(jnp.int32, (half, edge), 1)
    left, right = pl.ds(0, edge), pl.ds(edge, rest)

    def put(ref, slot, part, value):
        at = pl.ds(slot * half, half) if isinstance(slot, int) else pl.ds(pl.multiple_of(slot * half, half), half)
        ref[part, at, left] = jnp.where(column >= col, value, 0.0)
        ref[part, at, right] = jnp.where(column[:, :rest] < col, value[:, :rest], 0.0)

    by = lambda a, b: jnp.where(even, a, b)
    for q in range(edge // half):
        here = pl.ds(q * half, half)
        grad = cmul_conj(mult[0, here, :], mult[1, here, :], back[0, here, :], back[1, here, :])
        for part, value in enumerate(grad):
            if q == 0:
                put(keep, 4, part, jnp.where(line >= row, value, 0.0))
                put(keep, 3, part, jnp.where(line >= row, 0.0, value))
            elif q == 1:
                high = jnp.where(line + half >= row, 0.0, value)
                relay[part, :, :] = high
                put(send, by(4, 0), part, jnp.where(line + half >= row, value, 0.0))
                put(send, by(2, 4), part, high)
            elif q in (2, 5, 6):
                put(send, {2: by(3, 1), 5: by(0, 2), 6: by(1, 3)}[q], part, value)
            else:
                put(keep, {3: 0, 4: 1, 7: 2}[q], part, value)


def inward_kernel(place, own, partner, ahead, behind, swapped, far, light, turn, left, left_back, right, right_back, inner, field, moved):
    fill_window(place, own, partner, (ahead, None, behind, swapped, far), light, field, None)

    def propagate(rows, real, imag):
        put_field(moved, rows, *cmul(real, imag, turn[0, rows, :], turn[1, rows, :]))

    spectrum(field, left, right, False, propagate)

    def store(rows, real, imag):
        inner[0, rows, :] = real
        inner[1, rows, :] = imag

    spectrum(moved, left_back, right_back, True, store)


def turn_kernel(place, own, partner, top, bottom, behind, swapped, far, inner, amplitude, left, left_back, right, right_back, send, relay, keep, mid, field, moved, window, back):
    fill_window(place, own, partner, (top, bottom, behind, swapped, far), inner, field, window)

    def residual(rows, real, imag):
        modulus = jnp.sqrt(real * real + imag * imag)
        scale = 1.0 - amplitude[0, rows, :] / jnp.maximum(modulus, 0.1)
        put_field(moved, rows, real * scale, imag * scale)

    spectrum(field, left, right, False, residual)

    def store(rows, real, imag):
        back[0, rows, :] = real
        back[1, rows, :] = imag
        put_field(mid, rows, *cmul_conj(window[0, rows, :], window[1, rows, :], real, imag))

    spectrum(moved, left_back, right_back, True, store)
    put_pieces(place, inner, back, send, relay, keep)


def outward_kernel(place, mid, light, turn, left, left_back, right, right_back, send, relay, keep, moved, back):
    def propagate(rows, real, imag):
        put_field(moved, rows, *cmul_conj(turn[0, rows, :], turn[1, rows, :], real, imag))

    spectrum(mid, left, right, False, propagate)

    def store(rows, real, imag):
        back[0, rows, :] = real
        back[1, rows, :] = imag

    spectrum(moved, left_back, right_back, True, store)
    put_pieces(place, light, back, send, relay, keep)


def run(kernel, in_specs, arguments, out_shape, scratch):
    return pl.pallas_call(
        kernel,
        grid=(1,),
        in_specs=in_specs,
        out_specs=[pl.BlockSpec(x.shape, functools.partial(lambda n, i: (0,) * n, len(x.shape))) for x in out_shape],
        out_shape=out_shape,
        scratch_shapes=scratch,
        compiler_params=pltpu.CompilerParams(vmem_limit_bytes=16 << 20),
        cost_estimate=pl.CostEstimate(flops=4 << 30, bytes_accessed=16 << 20, transcendentals=0),
    )(*arguments)


def full(x):
    return pl.BlockSpec(x.shape, lambda i: (0,) * x.ndim)


def strip_of(k, x):
    return pl.BlockSpec((1,) + x.shape[1:], lambda i: (k, 0, 0, 0))


def piece_shapes(half, edge, cols):
    wide = jax.ShapeDtypeStruct((2, 5 * half, cols), jnp.float32)
    narrow = jax.ShapeDtypeStruct((2, half, edge), jnp.float32)
    return [wide, narrow, wide]


def after(value, *others):
    return lax.optimization_barrier((value,) + others)[0]


def widened(x, start, cols):
    edge = x.shape[2]
    rest = cols - edge
    column = lax.broadcasted_iota(jnp.int32, x.shape, 2)
    kept = jnp.where(column >= start, x, 0.0)
    wrapped = jnp.where(column < start, x, 0.0)[:, :, :rest]
    return jnp.concatenate([kept, wrapped], axis=2)


def narrowed(x, start, edge):
    rest = x.shape[2] - edge
    column = lax.broadcasted_iota(jnp.int32, x.shape[:2] + (rest,), 2)
    return jnp.concatenate(
        [jnp.where(column < start, x[:, :, edge:], x[:, :, :rest]), x[:, :, rest:edge]], axis=2
    )


def scattered(send, relay, keep, even, far_col, then):
    half = relay.shape[1]
    block = lambda x, slot: x[:, slot * half : (slot + 1) * half]
    far = hop(relay, lambda i: i + 1 if i % 2 == 1 else None)
    got = swap(send)
    to_bottom = block(keep, 3) + jnp.where(even, block(got, 3), 0.0)
    to_back = jnp.concatenate(
        [
            jnp.where(even, 0.0, block(got, 4)),
            block(keep, 4) + jnp.where(even, 0.0, block(got, 3)),
        ],
        axis=1,
    )
    mine = keep[:, : 2 * half] + got[:, : 2 * half]
    to_top = lambda far: block(keep, 2) + block(got, 2) + widened(far, far_col, keep.shape[2])
    if then is not None:
        to_ahead, then = lax.optimization_barrier((jnp.concatenate([to_top(far), to_bottom], axis=1), then))
        ahead = shift(to_ahead, 2)
    else:
        top = to_top(after(far, to_bottom, to_back))
        ahead = [shift(to_bottom, 2)]
        ahead = jnp.concatenate([shift(top, 2)] + ahead, axis=1)
    return mine + shift(to_back, -2) + ahead, then


def body(object_field, row_offset, col_offset, amplitudes, probe, phase):
    strip, cols = object_field.shape[2:]
    half = strip // 2
    edge = probe.shape[1]
    even = lax.rem(lax.axis_index("row"), 2) == 0
    place = jnp.stack([row_offset[0], col_offset[0], even.astype(jnp.int32)])

    lead = lax.optimization_barrier(object_field[0])
    rest_field = after(object_field, lead)
    ahead0 = shift(lead, -2)
    far_col = hop(col_offset, lambda i: i + 1 if i % 2 == 1 else None)[0]
    behind0 = shift(lead, 2)
    partner = swap(rest_field)
    turn = jnp.stack([jnp.cos(phase), jnp.sin(phase)])
    left, left_back, right, right_back, light = prepare(place, probe)

    def crossing(ahead, behind, even):
        top, bottom = ahead
        return jnp.concatenate(
            [top, jnp.where(even, jnp.concatenate([bottom, bottom], axis=1), behind)], axis=1
        )

    carried = lax.optimization_barrier(narrowed(ahead0[:, :half], far_col, edge))
    far0 = hop(carried, lambda i: i - 1 if i % 2 == 0 else None)
    later_field = after(rest_field, light)
    top1 = shift(later_field[1, :, :half], -2)
    bottom1 = shift(later_field[1, :, half:], -2)
    behind1 = shift(later_field[1], 2)
    swapped0 = swap(crossing((ahead0[:, :half], ahead0[:, half:]), behind0, after(even, carried)))

    waves = (left, left_back, right, right_back)
    smem = pl.BlockSpec(memory_space=pltpu.SMEM)
    square = jax.ShapeDtypeStruct((2, edge, edge), jnp.float32)
    field = jax.ShapeDtypeStruct((2 * edge, edge), jnp.bfloat16)
    scratch = [VMEM(x.shape, x.dtype) for x in (field, field, square, square)]

    parts = (ahead0, behind0, swapped0, far0)
    arguments = parts + (light, turn) + waves
    (inner,) = run(
        inward_kernel,
        [smem, strip_of(0, object_field), strip_of(0, partner)] + [full(x) for x in arguments],
        (place, object_field, partner) + arguments,
        [square],
        scratch[:2],
    )

    top1_after, even_after = lax.optimization_barrier((top1, even, inner))[:2]
    carried = narrowed(top1_after, far_col, edge)
    far1 = hop(carried, lambda i: i - 1 if i % 2 == 0 else None)
    swapped1 = swap(crossing((top1_after, bottom1), behind1, even_after))

    parts = (top1, bottom1, behind1, swapped1, far1)
    arguments = parts + (inner, amplitudes) + waves
    send, relay, keep, mid = run(
        turn_kernel,
        [smem, strip_of(1, object_field), strip_of(1, partner)] + [full(x) for x in arguments],
        (place, object_field, partner) + arguments,
        piece_shapes(half, edge, cols) + [field],
        scratch,
    )
    total2, mid = scattered(send, relay, keep, even, far_col, mid)

    arguments = (mid, light, turn) + waves
    send, relay, keep = run(
        outward_kernel,
        [smem] + [full(x) for x in arguments],
        (place,) + arguments,
        piece_shapes(half, edge, cols),
        [scratch[0], scratch[2]],
    )
    total1, _ = scattered(send, relay, keep, even, far_col, None)
    return object_field - 0.5 * jnp.stack([total1, total2])


def solution(mesh):
    placed = (
        P(None, None, ("scan", "row"), None),
        P(("scan", "row")),
        P(("scan", "row")),
        P(("scan", "row"), None, None),
        P("scan", None, None),
        P(),
    )
    return jax.shard_map(
        body,
        mesh=mesh,
        in_specs=placed,
        out_specs=P(None, None, ("scan", "row"), None),
        check_vma=False,
    )
```

```python
import functools
import math

import jax
import jax.numpy as jnp
from jax import lax
from jax.experimental import pallas as pl
from jax.experimental.pallas import tpu as pltpu
from jax.sharding import PartitionSpec as P


def hop(block, route):
    size = lax.axis_size("row")
    pairs = [(i, route(i) % size) for i in range(size) if route(i) is not None]
    return lax.ppermute(block, "row", pairs)


def shift(block, distance):
    return hop(block, lambda i: i + distance)


def swap(block):
    return hop(block, lambda i: i ^ 1)


VMEM = pltpu.VMEM
ROWS_AT_ONCE = 128


def cmul(a_real, a_imag, b_real, b_imag):
    return (a_real * b_real - a_imag * b_imag, a_real * b_imag + a_imag * b_real)


def cmul_conj(a_real, a_imag, b_real, b_imag):
    return (a_real * b_real + a_imag * b_imag, a_real * b_imag - a_imag * b_real)


def wave_table(count, step, edge):
    index = lax.broadcasted_iota(jnp.int32, (count, edge), 0) * step
    across = lax.broadcasted_iota(jnp.int32, (count, edge), 1)
    angles = lax.rem(index * across, edge).astype(jnp.float32) * (-2.0 * math.pi / edge)
    return jnp.cos(angles), jnp.sin(angles)


def prepare_kernel(place, far_col, probe, left, left_back, right, right_back, light, wraps, cos_base, sin_base):
    edge = probe.shape[1]
    fine = 32
    row, col = place[0], place[1]
    wraps[...] = (lax.broadcasted_iota(jnp.int32, wraps.shape, 1) < far_col[0]).astype(jnp.float32)
    factor = 1.0 / math.sqrt(edge)
    fine_cos, fine_sin = wave_table(fine, 1, edge)
    coarse_cos, coarse_sin = wave_table(edge // fine, fine, edge)
    for a in range(edge // fine):
        here = pl.ds(a * fine, fine)
        c, s = coarse_cos[a : a + 1], coarse_sin[a : a + 1]
        rounded = lambda x: (x * factor).astype(jnp.bfloat16).astype(jnp.float32)
        cos_base[here, :] = rounded(c * fine_cos - s * fine_sin)
        sin_base[here, :] = rounded(s * fine_cos + c * fine_sin)
    narrow = lambda x: x.astype(jnp.bfloat16)
    for part, base in enumerate((cos_base, sin_base)):
        here = pl.ds(part * edge, edge)
        left[part] = narrow(pltpu.roll(base[...], row, 1))
        left_back[part] = narrow(pltpu.roll(base[...], row, 0))
        right[here, :] = narrow(pltpu.roll(base[...], col, 0))
        right_back[here, :] = narrow(pltpu.roll(base[...], col, 1))
        light[part] = pltpu.roll(pltpu.roll(probe[part], row, 0), col, 1)


def whole(count):
    return [pl.BlockSpec(memory_space=VMEM)] * count


def prepare(place, far_col, probe, half):
    edge = probe.shape[1]
    pair = jax.ShapeDtypeStruct((2, edge, edge), jnp.bfloat16)
    tall = jax.ShapeDtypeStruct((2 * edge, edge), jnp.bfloat16)
    return pl.pallas_call(
        prepare_kernel,
        in_specs=[pl.BlockSpec(memory_space=pltpu.SMEM)] * 2 + whole(1),
        out_specs=whole(6),
        out_shape=[
            pair,
            pair,
            tall,
            tall,
            jax.ShapeDtypeStruct(probe.shape, jnp.float32),
            jax.ShapeDtypeStruct((half, edge), jnp.float32),
        ],
        scratch_shapes=[VMEM((edge, edge), jnp.float32)] * 2,
        compiler_params=pltpu.CompilerParams(vmem_limit_bytes=16 << 20),
        cost_estimate=pl.CostEstimate(flops=16 << 20, bytes_accessed=8 << 20, transcendentals=0),
        name="prepare",
    )(place, far_col, probe)


def spectrum(field, left, right, back, emit):
    edge = field.shape[1]
    count = ROWS_AT_ONCE

    @pl.loop(0, edge // count)
    def _(i):
        rows = pl.ds(pl.multiple_of(i * count, count), count)
        c, s = left[0, rows, :], left[1, rows, :]
        if back:
            lhs = [[c, s], [-s, c]]
        else:
            lhs = [[c, -s], [s, c]]
        join = lambda x: jnp.concatenate([jnp.concatenate(y, axis=1) for y in x], axis=0)
        both = jnp.dot(join(lhs), field[...], preferred_element_type=jnp.float32).astype(jnp.bfloat16)
        real, imag = both[:count], both[count:]
        if back:
            lhs = [[real, imag], [imag, -real]]
        else:
            lhs = [[real, -imag], [imag, real]]
        out = jnp.dot(join(lhs), right[...], preferred_element_type=jnp.float32)
        emit(rows, out[:count], out[count:])


def stacked_at(ref, rows):
    return pl.ds(pl.multiple_of(rows.start + ref.shape[1], ROWS_AT_ONCE), rows.size)


def put_field(ref, rows, real, imag):
    ref[rows, :] = real.astype(jnp.bfloat16)
    ref[stacked_at(ref, rows), :] = imag.astype(jnp.bfloat16)


def fill_window(place, own, partner, parts, mult, field, window):
    ahead_top, ahead_bottom, behind, swapped, far = parts
    edge = field.shape[1]
    half = far.shape[1]
    if ahead_bottom is None:
        ahead_top, ahead_bottom = (ahead_top.at[:, pl.ds(i * half, half), :] for i in range(2))
    first, second = swapped.at[:, pl.ds(0, half), :], swapped.at[:, pl.ds(half, 2 * half), :]
    row, col, even = place[0], place[1], place[2] == 1
    rest = ahead_top.shape[2] - edge
    line = lax.broadcasted_iota(jnp.int32, (half, edge), 0)
    column = lax.broadcasted_iota(jnp.int32, (half, rest), 1)
    top, bottom = pl.ds(0, half), pl.ds(half, half)

    def at(ref, part, where):
        x = ref[part, where, :] if len(ref.shape) == 3 else ref[0, part, where, :]
        return jnp.concatenate(
            [jnp.where(column < col, x[:, edge:], x[:, :rest]), x[:, rest:edge]], axis=1
        )

    def rows_of(q, part):
        pick = lambda a, b: jnp.where(even, a, b)
        if q == 0:
            return jnp.where(line >= row, at(behind, part, bottom), at(ahead_bottom, part, top))
        if q == 1:
            low = pick(at(second, part, top), at(partner, part, top))
            high = pick(at(first, part, top), far[part])
            return jnp.where(line + half >= row, low, high)
        if q == 2:
            return pick(at(second, part, bottom), at(partner, part, bottom))
        if q == 3:
            return at(own, part, top)
        if q == 4:
            return at(own, part, bottom)
        if q == 5:
            return pick(at(partner, part, top), at(first, part, top))
        if q == 6:
            return pick(at(partner, part, bottom), at(second, part, top))
        return at(ahead_top, part, top)

    for q in range(edge // half):
        here = pl.ds(q * half, half)
        real, imag = rows_of(q, 0), rows_of(q, 1)
        if window is not None:
            window[0, here, :] = real
            window[1, here, :] = imag
        out_real, out_imag = cmul(mult[0, here, :], mult[1, here, :], real, imag)
        field[here, :] = out_real.astype(jnp.bfloat16)
        field[pl.ds(edge + q * half, half), :] = out_imag.astype(jnp.bfloat16)


def put_pieces(place, mult, back, send, relay, keep):
    edge = back.shape[1]
    half = relay.shape[1]
    rest = keep.shape[2] - edge
    row, col, even = place[0], place[1], place[2] == 1
    line = lax.broadcasted_iota(jnp.int32, (half, edge), 0)
    column = lax.broadcasted_iota(jnp.int32, (half, edge), 1)
    left, right = pl.ds(0, edge), pl.ds(edge, rest)

    def put(ref, slot, part, value):
        at = pl.ds(slot * half, half) if isinstance(slot, int) else pl.ds(pl.multiple_of(slot * half, half), half)
        ref[part, at, left] = jnp.where(column >= col, value, 0.0)
        ref[part, at, right] = jnp.where(column[:, :rest] < col, value[:, :rest], 0.0)

    by = lambda a, b: jnp.where(even, a, b)
    for q in range(edge // half):
        here = pl.ds(q * half, half)
        grad = cmul_conj(mult[0, here, :], mult[1, here, :], back[0, here, :], back[1, here, :])
        for part, value in enumerate(grad):
            if q == 0:
                put(keep, 4, part, jnp.where(line >= row, value, 0.0))
                put(keep, 3, part, jnp.where(line >= row, 0.0, value))
            elif q == 1:
                high = jnp.where(line + half >= row, 0.0, value)
                relay[part, :, :] = high
                put(send, by(4, 0), part, jnp.where(line + half >= row, value, 0.0))
                put(send, by(2, 4), part, high)
            elif q in (2, 5, 6):
                put(send, {2: by(3, 1), 5: by(0, 2), 6: by(1, 3)}[q], part, value)
            else:
                put(keep, {3: 0, 4: 1, 7: 2}[q], part, value)


def inward_kernel(place, own, partner, ahead, behind, swapped, far, light, turn, left, left_back, right, right_back, inner, field, moved):
    fill_window(place, own, partner, (ahead, None, behind, swapped, far), light, field, None)

    def propagate(rows, real, imag):
        put_field(moved, rows, *cmul(real, imag, turn[0, rows, :], turn[1, rows, :]))

    spectrum(field, left, right, False, propagate)

    def store(rows, real, imag):
        inner[0, rows, :] = real
        inner[1, rows, :] = imag

    spectrum(moved, left_back, right_back, True, store)


def turn_kernel(place, own, partner, top, bottom, behind, swapped, far, inner, amplitude, left, left_back, right, right_back, send, relay, keep, mid, field, moved, window, back):
    fill_window(place, own, partner, (top, bottom, behind, swapped, far), inner, field, window)

    def residual(rows, real, imag):
        modulus = jnp.sqrt(real * real + imag * imag)
        scale = 1.0 - amplitude[0, rows, :] / jnp.maximum(modulus, 0.1)
        put_field(moved, rows, real * scale, imag * scale)

    spectrum(field, left, right, False, residual)

    def store(rows, real, imag):
        back[0, rows, :] = real
        back[1, rows, :] = imag
        put_field(mid, rows, *cmul_conj(window[0, rows, :], window[1, rows, :], real, imag))

    spectrum(moved, left_back, right_back, True, store)
    put_pieces(place, inner, back, send, relay, keep)


def outward_kernel(place, mid, light, turn, left, left_back, right, right_back, send, relay, keep, moved, back):
    def propagate(rows, real, imag):
        put_field(moved, rows, *cmul_conj(turn[0, rows, :], turn[1, rows, :], real, imag))

    spectrum(mid, left, right, False, propagate)

    def store(rows, real, imag):
        back[0, rows, :] = real
        back[1, rows, :] = imag

    spectrum(moved, left_back, right_back, True, store)
    put_pieces(place, light, back, send, relay, keep)


def run(kernel, in_specs, arguments, out_shape, scratch):
    return pl.pallas_call(
        kernel,
        grid=(1,),
        in_specs=in_specs,
        out_specs=[pl.BlockSpec(x.shape, functools.partial(lambda n, i: (0,) * n, len(x.shape))) for x in out_shape],
        out_shape=out_shape,
        scratch_shapes=scratch,
        compiler_params=pltpu.CompilerParams(vmem_limit_bytes=16 << 20),
        cost_estimate=pl.CostEstimate(flops=4 << 30, bytes_accessed=16 << 20, transcendentals=0),
    )(*arguments)


def full(x):
    return pl.BlockSpec(x.shape, lambda i: (0,) * x.ndim)


def strip_of(k, x):
    return pl.BlockSpec((1,) + x.shape[1:], lambda i: (k, 0, 0, 0))


def piece_shapes(half, edge, cols):
    wide = jax.ShapeDtypeStruct((2, 5 * half, cols), jnp.float32)
    narrow = jax.ShapeDtypeStruct((2, half, edge), jnp.float32)
    return [wide, narrow, wide]


def after(value, *others):
    return lax.optimization_barrier((value,) + others)[0]


def widened(x, wraps, cols):
    rest = cols - x.shape[2]
    kept = jnp.where(wraps == 0.0, x, 0.0)
    wrapped = jnp.where(wraps[:, :rest] == 0.0, 0.0, x[:, :, :rest])
    return jnp.concatenate([kept, wrapped], axis=2)


def narrowed(x, wraps, edge):
    rest = x.shape[2] - edge
    return jnp.concatenate(
        [jnp.where(wraps[:, :rest] == 0.0, x[:, :, :rest], x[:, :, edge:]), x[:, :, rest:edge]], axis=2
    )


def scattered(send, relay, keep, even, wraps, then):
    half = relay.shape[1]
    block = lambda x, slot: x[:, slot * half : (slot + 1) * half]
    got = swap(send)
    far = hop(relay, lambda i: i + 1 if i % 2 == 1 else None)
    to_bottom = block(keep, 3) + jnp.where(even, block(got, 3), 0.0)
    to_back = jnp.concatenate(
        [
            jnp.where(even, 0.0, block(got, 4)),
            block(keep, 4) + jnp.where(even, 0.0, block(got, 3)),
        ],
        axis=1,
    )
    mine = keep[:, : 2 * half] + got[:, : 2 * half]
    far = after(far, to_bottom, to_back)
    to_top = block(keep, 2) + block(got, 2) + widened(far, wraps, keep.shape[2])
    if then is not None:
        to_top, then = lax.optimization_barrier((to_top, then))
    bottom = shift(to_bottom, 2)
    top = shift(to_top, 2)
    return mine + shift(to_back, -2) + jnp.concatenate([top, bottom], axis=1), then


def body(object_field, row_offset, col_offset, amplitudes, probe, phase):
    strip, cols = object_field.shape[2:]
    half = strip // 2
    edge = probe.shape[1]
    even = lax.rem(lax.axis_index("row"), 2) == 0
    place = jnp.stack([row_offset[0], col_offset[0], even.astype(jnp.int32)])

    lead = lax.optimization_barrier(object_field[0])
    rest_field = after(object_field, lead)
    ahead0 = shift(lead, -2)
    far_col = hop(col_offset, lambda i: i + 1 if i % 2 == 1 else None)
    behind0 = shift(lead, 2)
    partner = swap(rest_field)
    turn = jnp.stack([jnp.cos(phase), jnp.sin(phase)])
    left, left_back, right, right_back, light, wraps = prepare(
        after(place, turn), far_col, probe, half
    )

    def crossing(ahead, behind, even):
        top, bottom = ahead
        return jnp.concatenate(
            [top, jnp.where(even, jnp.concatenate([bottom, bottom], axis=1), behind)], axis=1
        )

    carried = lax.optimization_barrier(narrowed(ahead0[:, :half], wraps, edge))
    far0 = hop(carried, lambda i: i - 1 if i % 2 == 0 else None)
    later_field = after(rest_field, light)
    top1 = shift(later_field[1, :, :half], -2)
    bottom1 = shift(later_field[1, :, half:], -2)
    behind1 = shift(later_field[1], 2)
    swapped0 = swap(crossing((ahead0[:, :half], ahead0[:, half:]), behind0, after(even, carried)))

    waves = (left, left_back, right, right_back)
    smem = pl.BlockSpec(memory_space=pltpu.SMEM)
    square = jax.ShapeDtypeStruct((2, edge, edge), jnp.float32)
    field = jax.ShapeDtypeStruct((2 * edge, edge), jnp.bfloat16)
    scratch = [VMEM(x.shape, x.dtype) for x in (field, field, square, square)]

    parts = (ahead0, behind0, swapped0, far0)
    arguments = parts + (light, turn) + waves
    (inner,) = run(
        inward_kernel,
        [smem, strip_of(0, object_field), strip_of(0, partner)] + [full(x) for x in arguments],
        (place, object_field, partner) + arguments,
        [square],
        scratch[:2],
    )

    top1_after, even_after = lax.optimization_barrier((top1, even, inner))[:2]
    carried = narrowed(top1_after, wraps, edge)
    far1 = hop(carried, lambda i: i - 1 if i % 2 == 0 else None)
    swapped1 = swap(crossing((top1_after, bottom1), behind1, even_after))

    parts = (top1, bottom1, behind1, swapped1, far1)
    arguments = parts + (inner, amplitudes) + waves
    send, relay, keep, mid = run(
        turn_kernel,
        [smem, strip_of(1, object_field), strip_of(1, partner)] + [full(x) for x in arguments],
        (place, object_field, partner) + arguments,
        piece_shapes(half, edge, cols) + [field],
        scratch,
    )
    total2, mid = scattered(send, relay, keep, even, wraps, mid)

    arguments = (mid, light, turn) + waves
    send, relay, keep = run(
        outward_kernel,
        [smem] + [full(x) for x in arguments],
        (place,) + arguments,
        piece_shapes(half, edge, cols),
        [scratch[0], scratch[2]],
    )
    total1, _ = scattered(send, relay, keep, even, wraps, None)
    return object_field - 0.5 * jnp.stack([total1, total2])


def solution(mesh):
    placed = (
        P(None, None, ("scan", "row"), None),
        P(("scan", "row")),
        P(("scan", "row")),
        P(("scan", "row"), None, None),
        P("scan", None, None),
        P(),
    )
    return jax.shard_map(
        body,
        mesh=mesh,
        in_specs=placed,
        out_specs=P(None, None, ("scan", "row"), None),
        check_vma=False,
    )
```
